512 devices in a mesh: groups: 2 (over y), chan: 32 (over z), dop: 4 (over x), sub: 2 (over core).
Axes of the slice: x: 4, y: 2, z: 32, core: 2. Of those that a mesh axis runs over, the one named last changes fastest.
The devices are a block of a 4x8x32 slice.
Arguments:
- power: bfloat16 [2, 512, 128, 8192], P(None, ('groups', 'chan', 'sub'), 'dop'), parts along dimension 1, may hold values from 0.049804688 to 20
- window: int32 [4, 2], P('groups'), parts along dimension 0, may hold values from 1 to 32, as said below
- calib_index: int32 [4, 256], P('groups', ('chan', 'sub')), parts along dimension 0, may hold values from 0 to 15
- calib_table: float32 [16], replicated, may hold values from 0.5 to 8
Outputs:
- test_ratio: float32 [2, 256, 8192], P(None, ('groups', 'dop'), ('chan', 'sub')), parts along dimension 1
The draws below stay inside these ranges and needn't reach their ends.
There are 2 independent parts, one for each index of `groups`. The reference program is written for one: setup_inputs(seed, part) draws one part's arguments, and reference() takes and returns one part's arrays. A program takes and returns all parts, laid end to end along the dimension named above; an argument that names none is the same for every part. Nothing has to cross between parts.
Inputs may be any that keep to these rules, and one draw needn't show every extreme that they name: window[c, 0] is the guard count, from 1 to 8; window[c, 1] is the reach, from 16 to 32; interval 0 has reach 32.
All inputs are finite; a program needn't handle non-finite values.
Results may differ from the reference program's by a relative error of at most 0.0003.
Values sent between devices are 32-bit elements; how exact they have to be, the bound alone decides.
No kernel may reach another device: no remote copies, remote signals or barrier semaphores. Data moves between devices by JAX's collectives and lax.ppermute only.
A program may use at most 64 MiB of HBM per device.

```python
import math
import jax
import jax.numpy as jnp

CH = 256
DOP = 128
CPIS = 2
HALO = 32
CALIB = 32
LEVELS = 16
RANGE = 8192


def draw_window(key, part):
    guard_key = jax.random.fold_in(key, 11)
    reach_key = jax.random.fold_in(key, 23)
    guard = jax.random.randint(guard_key, (CPIS,), 1, 9)
    reach = jax.random.randint(reach_key, (CPIS,), 16, HALO + 1)
    reach = reach.at[0].set(HALO)
    return jnp.stack([guard, reach], axis=1).astype(jnp.int32)


def place_ends(result, key, least, largest):
    longest = result.shape.index(max(result.shape))
    spots = []
    for shift in (0, 1):
        where = [jax.random.randint(jax.random.fold_in(key, axis), (), 0, length) for axis, length in enumerate(result.shape)]
        where[longest] = (where[longest] + shift) % result.shape[longest]
        spots.append(tuple(where))
    return result.at[spots[0]].set(least).at[spots[1]].set(largest)


def level_of(key, dims, split, least, largest):
    def one(axis_at, shards_of):
        steps = jax.random.uniform(jax.random.fold_in(jax.random.fold_in(key, 6), axis_at), (shards_of,), jnp.float32, least / len(split), largest / len(split))
        return jnp.repeat(jnp.exp(steps), dims[axis_at] // shards_of).reshape((-1,) + (1,) * (len(dims) - axis_at - 1))

    loudness = one(*split[0])
    for cut in split[1:]:
        loudness = loudness * one(*cut)
    return loudness


def setup_inputs(seed: int = 0, part: int = 0) -> dict:
    key_list = jax.random.split(jax.random.key(seed), 5)
    part_splits = jax.random.split(jax.random.fold_in(key_list[4], part), 5)
    return {
        "power": jnp.clip(jnp.exp(math.log(20.0) - 5.9953784 * jax.random.uniform(part_splits[0], (CPIS, CH, DOP, RANGE), jnp.float32) ** level_of(part_splits[0], (CPIS, CH, DOP, RANGE), ((1, 64), (2, 4)), -0.2, 0.2)), 0.049804688, 20.0).astype(jnp.bfloat16),
        "window": draw_window(jax.random.fold_in(jax.random.fold_in(key_list[4], part), 71), part),
        "calib_index": place_ends(jax.random.randint(part_splits[2], (CPIS, RANGE // CALIB), 0, LEVELS), jax.random.fold_in(part_splits[2], 1), 0, LEVELS - 1).astype(jnp.int32),
        "calib_table": jnp.clip(jnp.exp(jax.random.uniform(key_list[3], (LEVELS,), jnp.float32, math.log(0.5), math.log(8.0))), 0.5, 8.0),
    }


def reference(power, window, calib_index, calib_table):
    integrated = jnp.sum(power, axis=1, dtype=jnp.float32)
    guard = window[:, 0]
    reach = window[:, 1]
    padded = jnp.pad(integrated, ((0, 0), (0, 0), (HALO, HALO)))
    total = jnp.zeros(integrated.shape, jnp.float32)
    for offset in range(1, HALO + 1):
        weight = ((offset > guard) & (offset <= reach)).astype(jnp.float32)[:, None, None]
        right = padded[:, :, HALO + offset:HALO + offset + RANGE]
        left = padded[:, :, HALO - offset:HALO - offset + RANGE]
        total = total + weight * (right + left)
    noise = total / (2.0 * (reach - guard).astype(jnp.float32))[:, None, None]
    levels = jnp.arange(LEVELS, dtype=jnp.int32)
    onehot = (calib_index[:, :, None] == levels[None, None, :]).astype(jnp.float32)
    block_scale = jnp.sum(onehot * calib_table[None, None, :], axis=-1)
    scale = jnp.broadcast_to(block_scale[:, :, None], (CPIS, RANGE // CALIB, CALIB)).reshape(CPIS, RANGE)
    return integrated / (scale[:, None, :] * noise)
```

```python
import functools

import jax
import jax.numpy as jnp
from jax import lax
from jax.experimental import pallas as pl
from jax.experimental.pallas import tpu as pltpu
from jax.sharding import PartitionSpec as P

HALO = 32
CALIB = 32
NEAR = 4


def fold_kernel(cells, pieces, me_ref, power_ref, *refs):
    own, even, odd, two, other, held, sems = refs
    intervals, _, _, length = power_ref.shape
    width = length // pieces
    chip, core = me_ref[0], me_ref[1]
    copies = []
    for c in range(intervals):
        for p in range(pieces):
            k = c * pieces + p
            copy = pltpu.make_async_copy(
                power_ref.at[c, :, :, pl.ds(p * width, width)], held.at[k], sems.at[k]
            )
            copy.start()
            copies.append(copy)
    chips = width // (2 * cells)
    for c in range(intervals):
        for p in range(pieces):
            k = c * pieces + p
            copies[k].wait()
            for j in range(chips):
                target = p * chips + j
                slot = target // NEAR
                step = lax.rem(target - chip + 1024 * NEAR, NEAR)
                first = lax.rem(chip, 2) == 0
                sums = []
                for s in range(2):
                    at = (2 * j + s) * cells
                    block = held[k, :, :, at : at + cells].astype(jnp.float32)
                    sums.append(jnp.sum(block, axis=0))
                here = jnp.where(core == 0, sums[0], sums[1])
                there = jnp.where(core == 0, sums[1], sums[0])
                place = jnp.where(
                    step == 0, 0, jnp.where(step == 2, 3, jnp.where((step == 1) == first, 1, 2))
                )
                other[place, slot, c] = there

                @pl.when(place == 0)
                def _():
                    own[slot, c] = here

                @pl.when(place == 1)
                def _():
                    even[slot, c] = here

                @pl.when(place == 2)
                def _():
                    odd[slot, c] = here

                @pl.when(place == 3)
                def _():
                    two[slot, c] = here


def fold(power, chip, core, chips):
    intervals, channels, rows, length = power.shape
    cells = length // (2 * chips)
    slots = chips // NEAR
    pieces = 4
    part = jax.ShapeDtypeStruct((slots, intervals, rows, cells), jnp.float32)
    whole = jax.ShapeDtypeStruct((NEAR, slots, intervals, rows, cells), jnp.float32)
    vmem = pl.BlockSpec(memory_space=pltpu.VMEM)
    return pl.pallas_call(
        functools.partial(fold_kernel, cells, pieces),
        in_specs=[pl.BlockSpec(memory_space=pltpu.SMEM), pl.BlockSpec(memory_space=pltpu.HBM)],
        out_specs=[vmem] * 5,
        out_shape=[part] * 4 + [whole],
        scratch_shapes=[
            pltpu.VMEM((intervals * pieces, channels, rows, length // pieces), power.dtype),
            pltpu.SemaphoreType.DMA((intervals * pieces,)),
        ],
        compiler_params=pltpu.CompilerParams(vmem_limit_bytes=16 << 20),
        name="fold",
    )(jnp.stack([chip, core]).astype(jnp.int32), power)


def swap(x, axes, pairs):
    return lax.ppermute(x, axes, [(a, b) for a, b in pairs] + [(b, a) for a, b in pairs])


def body(power, window, calib_index, calib_table):
    n = lax.axis_size("chan")
    chip, core = lax.axis_index("chan"), lax.axis_index("sub")
    slots = n // NEAR
    half = slots // 2
    own, even, odd, two, other = fold(power, chip, core, n)
    got = lax.ppermute(other, "sub", [(0, 1), (1, 0)])
    own, even, odd = own + got[0], even + got[1], odd + got[2]
    low, high = two[:half] + got[3, :half], two[half:] + got[3, half:]
    ring = range(0, n, 2)
    even = swap(even, "chan", [(i, i + 1) for i in ring])
    odd = swap(odd, "chan", [(i + 1, (i + 2) % n) for i in ring])
    fours = range(0, n, 4)
    low = swap(low, "chan", [(i + k, i + k + 2) for i in fours for k in (0, 1)])
    high = swap(high, "chan", [(i + k + 2, (i + k + 4) % n) for i in fours for k in (0, 1)])
    near = own + even + odd + jnp.concatenate([low, high], axis=0)
    groups = [[NEAR * g + k for g in range(slots)] for k in range(NEAR)]
    far = lax.all_to_all(near, "chan", 0, 0, axis_index_groups=groups, tiled=True)
    strip = jnp.sum(far, axis=0)

    cells = strip.shape[2]
    left, right = strip[:, :, :HALO], strip[:, :, cells - HALO :]
    inner = swap(jnp.where(core == 0, right, left), ("chan", "sub"), [(2 * k, 2 * k + 1) for k in range(n)])
    outer = swap(jnp.where(core == 0, left, right), ("chan", "sub"), [(2 * k + 1, 2 * k + 2) for k in range(n - 1)])
    padded = jnp.concatenate(
        [jnp.where(core == 0, outer, inner), strip, jnp.where(core == 0, inner, outer)], axis=2
    )
    guard = window[:, 0]
    reach = window[:, 1]
    source = jnp.arange(cells + 2 * HALO, dtype=jnp.int32)[:, None]
    target = jnp.arange(cells, dtype=jnp.int32)[None, :]
    distance = jnp.abs(source - HALO - target)
    band_matrix = (
        (distance[None, :, :] > guard[:, None, None])
        & (distance[None, :, :] <= reach[:, None, None])
    ).astype(jnp.float32)
    total = jnp.einsum("cdj,cji->cdi", padded, band_matrix, precision=lax.Precision.HIGHEST)
    noise = total / (2.0 * (reach - guard).astype(jnp.float32))[:, None, None]
    levels = jnp.arange(calib_table.shape[0], dtype=jnp.int32)
    onehot = (calib_index[:, :, None] == levels[None, None, :]).astype(jnp.float32)
    block_scale = jnp.sum(onehot * calib_table[None, None, :], axis=-1)
    intervals, blocks = block_scale.shape
    scale = jnp.broadcast_to(block_scale[:, :, None], (intervals, blocks, CALIB)).reshape(
        intervals, cells
    )
    return strip / (scale[:, None, :] * noise)


def solution(mesh):
    placed = (
        P(None, ("groups", "chan", "sub"), "dop", None),
        P("groups", None),
        P("groups", ("chan", "sub")),
        P(),
    )
    return jax.shard_map(
        body,
        mesh=mesh,
        in_specs=placed,
        out_specs=P(None, ("groups", "dop"), ("chan", "sub")),
        check_vma=False,
    )
```

```python
import functools

import jax
import jax.numpy as jnp
from jax import lax
from jax.experimental import pallas as pl
from jax.experimental.pallas import tpu as pltpu
from jax.sharding import PartitionSpec as P


HALO = 32
CALIB = 32
NEAR = 4
FAR_ORDER = (0, 4, 6, 7, 2, 1, 3, 5)


def far_order(slots):
    return list(FAR_ORDER if len(FAR_ORDER) == slots else range(slots))


def fold_kernel(cells, order, pieces, me_ref, power_ref, *refs):
    own, even, odd, two, other, held, sems = refs
    intervals, _, _, length = power_ref.shape
    width = length // pieces
    chip, core = me_ref[0], me_ref[1]
    copies = []
    for c in range(intervals):
        for p in range(pieces):
            k = c * pieces + p
            copy = pltpu.make_async_copy(
                power_ref.at[c, :, :, pl.ds(p * width, width)], held.at[k], sems.at[k]
            )
            copy.start()
            copies.append(copy)
    chips = width // (2 * cells)
    for c in range(intervals):
        for p in range(pieces):
            k = c * pieces + p
            copies[k].wait()
            for j in range(chips):
                target = p * chips + j
                slot = order.index(target // NEAR)
                step = lax.rem(target - chip + 1024 * NEAR, NEAR)
                first = lax.rem(chip, 2) == 0
                sums = []
                for s in range(2):
                    at = (2 * j + s) * cells
                    block = held[k, :, :, at : at + cells].astype(jnp.float32)
                    sums.append(jnp.sum(block, axis=0))
                here = jnp.where(core == 0, sums[0], sums[1])
                there = jnp.where(core == 0, sums[1], sums[0])
                place = jnp.where(
                    step == 0, 0, jnp.where(step == 2, 3, jnp.where((step == 1) == first, 1, 2))
                )
                other[place, slot, c] = there

                @pl.when(place == 0)
                def _():
                    own[slot, c] = here

                @pl.when(place == 1)
                def _():
                    even[slot, c] = here

                @pl.when(place == 2)
                def _():
                    odd[slot, c] = here

                @pl.when(place == 3)
                def _():
                    two[slot, c] = here


def fold(power, chip, core, chips):
    intervals, channels, rows, length = power.shape
    cells = length // (2 * chips)
    slots = chips // NEAR
    pieces = 4
    part = jax.ShapeDtypeStruct((slots, intervals, rows, cells), jnp.float32)
    whole = jax.ShapeDtypeStruct((NEAR, slots, intervals, rows, cells), jnp.float32)
    vmem = pl.BlockSpec(memory_space=pltpu.VMEM)
    return pl.pallas_call(
        functools.partial(fold_kernel, cells, far_order(slots), pieces),
        in_specs=[pl.BlockSpec(memory_space=pltpu.SMEM), pl.BlockSpec(memory_space=pltpu.HBM)],
        out_specs=[vmem] * 5,
        out_shape=[part] * 4 + [whole],
        scratch_shapes=[
            pltpu.VMEM((intervals * pieces, channels, rows, length // pieces), power.dtype),
            pltpu.SemaphoreType.DMA((intervals * pieces,)),
        ],
        compiler_params=pltpu.CompilerParams(vmem_limit_bytes=50 << 20),
        name="fold",
    )(jnp.stack([chip, core]).astype(jnp.int32), power)


def swap(x, axes, pairs):
    return lax.ppermute(x, axes, [(a, b) for a, b in pairs] + [(b, a) for a, b in pairs])


def body(power, window, calib_index, calib_table):
    n = lax.axis_size("chan")
    chip, core = lax.axis_index("chan"), lax.axis_index("sub")
    slots = n // NEAR
    half = slots // 2
    own, even, odd, two, other = fold(power, chip, core, n)
    got = lax.ppermute(other, "sub", [(0, 1), (1, 0)])
    own, even, odd = own + got[0], even + got[1], odd + got[2]
    low, high = two[:half] + got[3, :half], two[half:] + got[3, half:]
    ring = range(0, n, 2)
    fours = range(0, n, 4)
    even = swap(even, "chan", [(i, i + 1) for i in ring])
    odd = swap(odd, "chan", [(i + 1, (i + 2) % n) for i in ring])
    low = swap(low, "chan", [(i + k, i + k + 2) for i in fours for k in (0, 1)])
    high = swap(high, "chan", [(i + k + 2, (i + k + 4) % n) for i in fours for k in (0, 1)])
    near = own + even + odd + jnp.concatenate([low, high], axis=0)
    groups = [[NEAR * g + k for g in far_order(slots)] for k in range(NEAR)]
    far = lax.all_to_all(near, "chan", 0, 0, axis_index_groups=groups, tiled=True)
    strip = jnp.sum(far, axis=0)

    cells = strip.shape[2]
    left, right = strip[:, :, :HALO], strip[:, :, cells - HALO :]
    inner = swap(jnp.where(core == 0, right, left), ("chan", "sub"), [(2 * k, 2 * k + 1) for k in range(n)])
    outer = swap(jnp.where(core == 0, left, right), ("chan", "sub"), [(2 * k + 1, 2 * k + 2) for k in range(n - 1)])
    padded = jnp.concatenate(
        [jnp.where(core == 0, outer, inner), strip, jnp.where(core == 0, inner, outer)], axis=2
    )
    guard = window[:, 0]
    reach = window[:, 1]
    source = jnp.arange(cells + 2 * HALO, dtype=jnp.int32)[:, None]
    target = jnp.arange(cells, dtype=jnp.int32)[None, :]
    distance = jnp.abs(source - HALO - target)
    band_matrix = (
        (distance[None, :, :] > guard[:, None, None])
        & (distance[None, :, :] <= reach[:, None, None])
    ).astype(jnp.float32)
    total = jnp.einsum("cdj,cji->cdi", padded, band_matrix, precision=lax.Precision.HIGHEST)
    noise = total / (2.0 * (reach - guard).astype(jnp.float32))[:, None, None]
    levels = jnp.arange(calib_table.shape[0], dtype=jnp.int32)
    onehot = (calib_index[:, :, None] == levels[None, None, :]).astype(jnp.float32)
    block_scale = jnp.sum(onehot * calib_table[None, None, :], axis=-1)
    intervals, blocks = block_scale.shape
    scale = jnp.broadcast_to(block_scale[:, :, None], (intervals, blocks, CALIB)).reshape(
        intervals, cells
    )
    return strip / (scale[:, None, :] * noise)


def solution(mesh):
    placed = (
        P(None, ("groups", "chan", "sub"), "dop", None),
        P("groups", None),
        P("groups", ("chan", "sub")),
        P(),
    )
    return jax.shard_map(
        body,
        mesh=mesh,
        in_specs=placed,
        out_specs=P(None, ("groups", "dop"), ("chan", "sub")),
        check_vma=False,
    )
```

```python
import functools

import jax
import jax.numpy as jnp
from jax import lax
from jax.experimental import pallas as pl
from jax.experimental.pallas import tpu as pltpu
from jax.sharding import PartitionSpec as P


HALO = 32
CALIB = 32
NEAR = 4
FAR_ORDER = (0, 4, 6, 7, 2, 1, 3, 5)


def far_order(slots):
    return list(FAR_ORDER if len(FAR_ORDER) == slots else range(slots))


def fold_kernel(cells, order, pieces, me_ref, power_ref, mine, other, held, sems):
    intervals, _, _, length = power_ref.shape
    width = length // pieces
    chip, core = me_ref[0], me_ref[1]
    copies = []
    for c in range(intervals):
        for p in range(pieces):
            k = c * pieces + p
            copy = pltpu.make_async_copy(
                power_ref.at[c, :, :, pl.ds(p * width, width)], held.at[k], sems.at[k]
            )
            copy.start()
            copies.append(copy)
    first = lax.rem(chip, 2) == 0
    chips = width // (2 * cells)
    for c in range(intervals):
        for p in range(pieces):
            k = c * pieces + p
            copies[k].wait()
            for j in range(chips):
                target = p * chips + j
                slot = order.index(target // NEAR)
                step = lax.rem(target - chip + 1024 * NEAR, NEAR)
                place = jnp.where(
                    step == 0, 0, jnp.where(step == 2, 3, jnp.where((step == 1) == first, 1, 2))
                )
                for side, out in ((core, mine), (1 - core, other)):
                    start = pl.multiple_of((2 * j + side) * cells, cells)
                    block = held[k, :, :, pl.ds(start, cells)].astype(jnp.float32)
                    out[place, slot, c] = jnp.sum(block, axis=0)


def fold(power, chip, core, chips):
    intervals, channels, rows, length = power.shape
    cells = length // (2 * chips)
    slots = chips // NEAR
    pieces = 8
    strips = jax.ShapeDtypeStruct((NEAR, slots, intervals, rows, cells), jnp.float32)
    vmem = pl.BlockSpec(memory_space=pltpu.VMEM)
    return pl.pallas_call(
        functools.partial(fold_kernel, cells, far_order(slots), pieces),
        in_specs=[pl.BlockSpec(memory_space=pltpu.SMEM), pl.BlockSpec(memory_space=pl.ANY)],
        out_specs=[vmem, vmem],
        out_shape=[strips, strips],
        scratch_shapes=[
            pltpu.VMEM((intervals * pieces, channels, rows, length // pieces), power.dtype),
            pltpu.SemaphoreType.DMA((intervals * pieces,)),
        ],
        compiler_params=pltpu.CompilerParams(vmem_limit_bytes=50 << 20),
        name="fold",
    )(jnp.stack([chip, core]).astype(jnp.int32), power)


def swap(x, axes, pairs):
    return lax.ppermute(x, axes, [(a, b) for a, b in pairs] + [(b, a) for a, b in pairs])


def body(power, window, calib_index, calib_table):
    n = lax.axis_size("chan")
    chip, core = lax.axis_index("chan"), lax.axis_index("sub")
    slots = n // NEAR
    half = slots // 2
    mine, other = fold(power, chip, core, n)
    got = lax.ppermute(other, "sub", [(0, 1), (1, 0)])
    own, even, odd = mine[0] + got[0], mine[1] + got[1], mine[2] + got[2]
    low, high = mine[3, :half] + got[3, :half], mine[3, half:] + got[3, half:]
    ring = range(0, n, 2)
    fours = range(0, n, 4)
    even = swap(even, "chan", [(i, i + 1) for i in ring])
    odd = swap(odd, "chan", [(i + 1, (i + 2) % n) for i in ring])
    low = swap(low, "chan", [(i + k, i + k + 2) for i in fours for k in (0, 1)])
    high = swap(high, "chan", [(i + k + 2, (i + k + 4) % n) for i in fours for k in (0, 1)])
    near = lax.optimization_barrier(own + even + jnp.concatenate([low, high], axis=0)) + odd
    groups = [[NEAR * g + k for g in far_order(slots)] for k in range(NEAR)]
    far = lax.all_to_all(near, "chan", 0, 0, axis_index_groups=groups, tiled=True)
    strip = jnp.sum(far, axis=0)

    cells = strip.shape[2]
    left, right = strip[:, :, :HALO], strip[:, :, cells - HALO :]
    inner = swap(jnp.where(core == 0, right, left), ("chan", "sub"), [(2 * k, 2 * k + 1) for k in range(n)])
    outer = swap(jnp.where(core == 0, left, right), ("chan", "sub"), [(2 * k + 1, 2 * k + 2) for k in range(n - 1)])
    padded = jnp.concatenate(
        [jnp.where(core == 0, outer, inner), strip, jnp.where(core == 0, inner, outer)], axis=2
    )
    guard = window[:, 0]
    reach = window[:, 1]
    source = jnp.arange(cells + 2 * HALO, dtype=jnp.int32)[:, None]
    target = jnp.arange(cells, dtype=jnp.int32)[None, :]
    distance = jnp.abs(source - HALO - target)
    band_matrix = (
        (distance[None, :, :] > guard[:, None, None])
        & (distance[None, :, :] <= reach[:, None, None])
    ).astype(jnp.float32)
    total = jnp.einsum("cdj,cji->cdi", padded, band_matrix, precision=lax.Precision.HIGHEST)
    noise = total / (2.0 * (reach - guard).astype(jnp.float32))[:, None, None]
    levels = jnp.arange(calib_table.shape[0], dtype=jnp.int32)
    onehot = (calib_index[:, :, None] == levels[None, None, :]).astype(jnp.float32)
    block_scale = jnp.sum(onehot * calib_table[None, None, :], axis=-1)
    intervals, blocks = block_scale.shape
    scale = jnp.broadcast_to(block_scale[:, :, None], (intervals, blocks, CALIB)).reshape(
        intervals, cells
    )
    return strip / (scale[:, None, :] * noise)


def solution(mesh):
    placed = (
        P(None, ("groups", "chan", "sub"), "dop", None),
        P("groups", None),
        P("groups", ("chan", "sub")),
        P(),
    )
    return jax.shard_map(
        body,
        mesh=mesh,
        in_specs=placed,
        out_specs=P(None, ("groups", "dop"), ("chan", "sub")),
        check_vma=False,
    )
```
